16 devices in a mesh: dp: 4 (over z, y), tp: 4 (over x, core).
Axes of the slice: x: 2, y: 2, z: 2, core: 2. Of those that a mesh axis runs over, the one named last changes fastest.
Arguments:
- hidden: bfloat16 [4, 2048, 6144], P('dp', 'tp'), parts along dimension 0
- attn_gain: float32 [6144], replicated
- attn_bias: float32 [6144], replicated
- mlp_gain: float32 [6144], replicated
- mlp_bias: float32 [6144], replicated
- w_qkv: bfloat16 [6144, 64, 288], P(None, 'tp')
- w_out: bfloat16 [6144, 6144], P('tp')
- w_up: bfloat16 [6144, 24576], P(None, 'tp')
- w_down: bfloat16 [24576, 6144], P('tp')
- positions: int32 [2048], replicated
Outputs:
- output: bfloat16 [4, 2048, 6144], P('dp', 'tp'), parts along dimension 0
There are 4 independent parts. The reference program is written for one: setup_inputs(seed, part) draws one part's arguments, and reference() takes and returns one part's arrays. A program takes and returns all parts, laid end to end along the dimension named above; an argument that names none is the same for every part.
All inputs are finite; a program needn't handle non-finite values.
Results may differ from the reference program's by a relative error of at most 0.00619968.
Values are sent between devices in bfloat16 or wider.
A program may use at most 1 GiB of HBM per device.

```python
import jax
import jax.numpy as jnp
from jax import lax

D = 6144
HEADS = 64
KV_HEADS = 64
HEAD = 96
FF = 24576
BATCH = 1
SEQ_LEN = 2048
QUERY_BLOCK = 64
HALF_HEAD = 48

GROUP_SIZE = HEADS // KV_HEADS
QKV_COLS = (GROUP_SIZE + 2) * HEAD


def setup_inputs(seed: int = 0, part: int = 0) -> dict:
    root_key = jax.random.key(seed)
    sub_keys = jax.random.split(root_key, 10)
    part_key = jax.random.fold_in(sub_keys[0], part)
    hidden = jax.random.normal(part_key, (BATCH, SEQ_LEN, D), jnp.float32).astype(jnp.bfloat16)
    attn_gain = 1.0 + 0.4 * jax.random.normal(sub_keys[1], (D,), jnp.float32)
    attn_bias = 0.4 * jax.random.normal(sub_keys[2], (D,), jnp.float32)
    mlp_gain = 1.0 + 0.4 * jax.random.normal(sub_keys[3], (D,), jnp.float32)
    mlp_bias = 0.4 * jax.random.normal(sub_keys[4], (D,), jnp.float32)
    w_qkv = (1.2 * D ** -0.5 * jax.random.normal(sub_keys[5], (D, KV_HEADS, QKV_COLS), jnp.float32)).astype(jnp.bfloat16)
    w_out = (2.0 * (HEADS * HEAD) ** -0.5 * jax.random.normal(sub_keys[6], (HEADS * HEAD, D), jnp.float32)).astype(jnp.bfloat16)
    w_up = (D ** -0.5 * jax.random.normal(sub_keys[7], (D, FF), jnp.float32)).astype(jnp.bfloat16)
    w_down = (FF ** -0.5 * jax.random.normal(sub_keys[8], (FF, D), jnp.float32)).astype(jnp.bfloat16)
    pos_gaps = jax.random.randint(sub_keys[9], (SEQ_LEN,), 1, 4, jnp.int32)
    positions = (jnp.cumsum(pos_gaps) - pos_gaps[0]).astype(jnp.int32)
    return {'hidden': hidden, 'attn_gain': attn_gain, 'attn_bias': attn_bias, 'mlp_gain': mlp_gain, 'mlp_bias': mlp_bias, 'w_qkv': w_qkv, 'w_out': w_out, 'w_up': w_up, 'w_down': w_down, 'positions': positions}


def layer_norm(tok_rows, norm_gain, norm_bias):
    rows32 = tok_rows.astype(jnp.float32)
    row_mean = jnp.mean(rows32, axis=-1, keepdims=True)
    centered = rows32 - row_mean
    row_var = jnp.mean(centered * centered, axis=-1, keepdims=True)
    return (centered * lax.rsqrt(row_var + 1e-5) * norm_gain + norm_bias).astype(jnp.bfloat16)


def apply_rotary(head_vals, cos_tab, sin_tab):
    vals32 = head_vals.astype(jnp.float32)
    rotated = jnp.concatenate([-vals32[..., HALF_HEAD:], vals32[..., :HALF_HEAD]], axis=-1)
    return (vals32 * cos_tab + rotated * sin_tab).astype(jnp.bfloat16)


def attend_sequence(query_rot, key_rot, value_seq):
    key32 = key_rot.astype(jnp.float32)
    value32 = value_seq.astype(jnp.float32)
    key_idx = jnp.arange(SEQ_LEN)

    def one_block(block_idx):
        row_start = block_idx * QUERY_BLOCK
        query_blk = lax.dynamic_slice_in_dim(query_rot, row_start, QUERY_BLOCK, axis=0).astype(jnp.float32)
        scores = jnp.einsum('qkgh,skh->kgqs', query_blk, key32) * HEAD ** -0.5
        query_idx = row_start + jnp.arange(QUERY_BLOCK)
        allowed = key_idx[None, :] <= query_idx[:, None]
        scores = jnp.where(allowed, scores, -1e30)
        exp_scores = jnp.exp(scores - jnp.max(scores, axis=-1, keepdims=True))
        attn_probs = (exp_scores / jnp.sum(exp_scores, axis=-1, keepdims=True)).astype(jnp.bfloat16)
        context = jnp.einsum('kgqs,skh->qkgh', attn_probs.astype(jnp.float32), value32)
        return context.astype(jnp.bfloat16)

    ctx_blocks = lax.map(one_block, jnp.arange(SEQ_LEN // QUERY_BLOCK))
    return ctx_blocks.reshape(SEQ_LEN, HEADS * HEAD)


def reference(hidden, attn_gain, attn_bias, mlp_gain, mlp_bias, w_qkv, w_out, w_up, w_down, positions):
    inv_freq = 10000.0 ** (-2.0 * jnp.arange(HALF_HEAD, dtype=jnp.float32) / HEAD)
    angles = positions.astype(jnp.float32)[:, None] * inv_freq[None, :]
    angles = jnp.concatenate([angles, angles], axis=-1)
    cos_tab = jnp.cos(angles)
    sin_tab = jnp.sin(angles)
    w_qkv_flat = w_qkv.reshape(D, KV_HEADS * QKV_COLS)

    def one_sequence(seq_rows):
        normed_attn = layer_norm(seq_rows, attn_gain, attn_bias)
        normed_mlp = layer_norm(seq_rows, mlp_gain, mlp_bias)
        qkv_rows = jnp.dot(normed_attn, w_qkv_flat, preferred_element_type=jnp.float32).astype(jnp.bfloat16)
        qkv_rows = qkv_rows.reshape(SEQ_LEN, KV_HEADS, GROUP_SIZE + 2, HEAD)
        query_rot = apply_rotary(qkv_rows[:, :, :GROUP_SIZE, :], cos_tab[:, None, None, :], sin_tab[:, None, None, :])
        key_rot = apply_rotary(qkv_rows[:, :, GROUP_SIZE, :], cos_tab[:, None, :], sin_tab[:, None, :])
        value_seq = qkv_rows[:, :, GROUP_SIZE + 1, :]
        context = attend_sequence(query_rot, key_rot, value_seq)
        attn_part = jnp.dot(context, w_out, preferred_element_type=jnp.float32)
        up_pre = jnp.dot(normed_mlp, w_up, preferred_element_type=jnp.float32)
        up_act = jax.nn.gelu(up_pre, approximate=False).astype(jnp.bfloat16)
        mlp_part = jnp.dot(up_act, w_down, preferred_element_type=jnp.float32)
        return (seq_rows.astype(jnp.float32) + attn_part + mlp_part).astype(jnp.bfloat16)

    return lax.map(one_sequence, hidden)
```

```python
import functools

import jax
import jax.numpy as jnp
from jax import lax
from jax.experimental import pallas as pl
from jax.experimental.pallas import tpu as pltpu
from jax.sharding import PartitionSpec as P

F32 = jnp.float32
BF16 = jnp.bfloat16
VMEM_LIMIT = 67_000_000
LOG2E = 1.4426950408889634


def rotary_tables(positions, half_dim):
    inv_freq = 10000.0 ** (-2.0 * jnp.arange(half_dim, dtype=F32) / (2 * half_dim))
    angles = inv_freq[:, None] * positions.astype(F32)[None, :]
    return jnp.cos(angles), jnp.sin(angles)


def peers():
    tp = lax.axis_index('tp')
    mate = tp + 1 - 2 * lax.rem(tp, 2)
    cross = lax.rem(tp + 2, 4)
    return mate, cross


def entry_barrier(mate, cross):
    sem = pltpu.get_barrier_semaphore()
    for dev in (mate, cross):
        pl.semaphore_signal(sem, inc=1, device_id={'tp': dev}, device_id_type=pl.DeviceIdType.MESH)
    pl.semaphore_wait(sem, 2)


def gelu(pre):
    return pre * (lax.erf(pre * (2.0 ** -0.5)) + 1.0) * 0.5


def norm_rows(width, x_s, a_s, m_s, ga, ba, gm, bm):
    tall, wide = 64, 512
    span = width // wide

    def lanes(j):
        return pl.ds(pl.multiple_of(j * wide, wide), wide)

    def fold(v):
        return sum(v[:, k:k + 128] for k in range(0, wide, 128))

    def chunk(i, carry):
        at = pl.ds(pl.multiple_of(i * tall, tall), tall)
        zero = jnp.zeros((tall, 128), F32)
        tot = lax.fori_loop(0, span, lambda j, acc: acc + fold(x_s[at, lanes(j)].astype(F32)), zero)
        mean = jnp.sum(tot, axis=-1, keepdims=True) * (1.0 / width)

        def square(j, acc):
            c = x_s[at, lanes(j)].astype(F32) - mean
            return acc + fold(c * c)

        var = jnp.sum(lax.fori_loop(0, span, square, zero), axis=-1, keepdims=True) * (1.0 / width)
        inv = lax.rsqrt(var + 1e-5)

        def write(j, acc):
            z = (x_s[at, lanes(j)].astype(F32) - mean) * inv
            a_s[at, lanes(j)] = (z * ga[:, lanes(j)] + ba[:, lanes(j)]).astype(BF16)
            m_s[at, lanes(j)] = (z * gm[:, lanes(j)] + bm[:, lanes(j)]).astype(BF16)
            return acc

        return lax.fori_loop(0, span, write, carry)

    lax.fori_loop(0, x_s.shape[0] // tall, chunk, 0)


def front_kernel(nq, nu, x_hbm, wq_ref, wu_ref, ga, ba, gm, bm, qkv_ref, act_ref, xr, x_s, a_s, m_s, pre_s, load_sem, send_sem, recv_sem):
    r, t = pl.program_id(0), pl.program_id(1)
    nt = nq + nu
    even = lax.rem(r, 2) == 0
    is_q = jnp.logical_or(jnp.logical_and(even, t < nq), jnp.logical_and(jnp.logical_not(even), t >= nu))
    mate, cross = peers()
    rows, width = x_s.shape

    def remote(k):
        src = x_hbm if k < 2 else xr.at[1]
        dev = cross if k == 1 else mate
        return pltpu.make_async_remote_copy(src_ref=src, dst_ref=xr.at[k], send_sem=send_sem.at[k], recv_sem=recv_sem.at[k], device_id={'tp': dev}, device_id_type=pl.DeviceIdType.MESH)

    def load(k):
        return pltpu.make_async_copy(x_hbm if k < 0 else xr.at[k], x_s, load_sem)

    @pl.when(jnp.logical_and(r == 0, t == 0))
    def _():
        load(-1).start()
        entry_barrier(mate, cross)
        remote(1).start()
        remote(0).start()

    @pl.when(t == 0)
    def _():
        load(-1).wait()

        norm_rows(width, x_s, a_s, m_s, ga, ba, gm, bm)

    @pl.when(is_q)
    def _():
        qkv_ref[...] = lax.dot_general(wq_ref[...], a_s[...], (((1,), (1,)), ((), ())), preferred_element_type=F32).astype(BF16)

    @pl.when(jnp.logical_not(is_q))
    def _():
        cols = wu_ref.shape[1]
        for c in range(0, cols, 256):
            at = slice(c, c + 256)
            act_ref[:, at] = gelu(pre_s[:, at]).astype(BF16)
            pre_s[:, at] = jnp.dot(m_s[...], wu_ref[:, at], preferred_element_type=F32)

    for k in range(3):
        @pl.when(jnp.logical_and(r == k, t == nt - 2))
        def _():
            remote(k).wait_recv()
            load(k).start()
            if k == 1:
                remote(2).start()

    @pl.when(jnp.logical_and(r == 3, t == nt - 1))
    def _():
        act_ref[...] = gelu(pre_s[...]).astype(BF16)
        for k in range(3):
            remote(k).wait_send()


def front(x, wq, wu, ga, ba, gm, bm):
    rows, width = x.shape
    qcols, ff = wq.shape[0], wu.shape[1]
    tq, tu = 512, 512
    nq, nu = qcols // tq, ff // tu
    nt = nq + nu

    def even(r):
        return lax.rem(r, 2) == 0

    def wq_at(r, t):
        return jnp.where(even(r), jnp.minimum(t, nq - 1), jnp.minimum(nq - 1, nt - 1 - t)), 0

    def wu_at(r, t):
        return 0, jnp.where(even(r), jnp.maximum(t - nq, 0), jnp.maximum(nu - 1 - t, 0))

    def qkv_at(r, t):
        held = jnp.logical_and(jnp.logical_not(even(r)), t < nu)
        return wq_at(r, t)[0], jnp.where(held, r - 1, r)

    def act_at(r, t):
        done = jnp.where(even(r), r * nu + jnp.maximum(t - nq + 1, 0), r * nu + jnp.minimum(t + 1, nu))
        idx = jnp.maximum(done - 2, 0)
        idx = jnp.where(jnp.logical_and(r == 3, t == nt - 1), 4 * nu - 1, idx)
        blk, k = lax.div(idx, nu), lax.rem(idx, nu)
        return blk, jnp.where(even(blk), k, nu - 1 - k)

    vec = pl.BlockSpec((1, width), lambda r, t: (0, 0))
    flops = 2 * 4 * rows * width * (qcols + ff)
    return pl.pallas_call(
        functools.partial(front_kernel, nq, nu),
        grid=(4, nt),
        out_shape=(jax.ShapeDtypeStruct((qcols, 4 * rows), BF16), jax.ShapeDtypeStruct((4 * rows, ff), BF16), jax.ShapeDtypeStruct((3, rows, width), BF16)),
        in_specs=[pl.BlockSpec(memory_space=pl.ANY), pl.BlockSpec((tq, width), wq_at), pl.BlockSpec((width, tu), wu_at), vec, vec, vec, vec],
        out_specs=(pl.BlockSpec((tq, rows), qkv_at), pl.BlockSpec((rows, tu), act_at), pl.BlockSpec(memory_space=pl.ANY)),
        scratch_shapes=[
            pltpu.VMEM((rows, width), BF16),
            pltpu.VMEM((rows, width), BF16),
            pltpu.VMEM((rows, width), BF16),
            pltpu.VMEM((rows, tu), F32),
            pltpu.SemaphoreType.DMA,
            pltpu.SemaphoreType.DMA((3,)),
            pltpu.SemaphoreType.DMA((3,)),
        ],
        compiler_params=pltpu.CompilerParams(collective_id=0, has_side_effects=True, vmem_limit_bytes=VMEM_LIMIT, dimension_semantics=('arbitrary', 'arbitrary')),
        cost_estimate=pl.CostEstimate(flops=flops, bytes_accessed=4 * 2 * width * (qcols + ff), transcendentals=0),
        name='front',
    )(x, wq, wu, ga, ba, gm, bm)[:2]


def attn_kernel(scale, heads_out, tp_ref, qkv_ref, cos_ref, sin_ref, ctx_ref, q_s, k_s, v_s, s_s, p_s, c_s):
    g = pl.program_id(0)
    tp = tp_ref[0]
    half, seq = cos_ref.shape
    hd = 2 * half
    blk = seq // 4
    pad = k_s.shape[1]

    def rel(j):
        return pl.multiple_of((tp ^ j) * blk, blk)

    def rotate(base, j):
        at = pl.ds(rel(j), blk)
        u1 = qkv_ref[base:base + half, at].astype(F32)
        u2 = qkv_ref[base + half:base + hd, at].astype(F32)
        c, s = cos_ref[:, j * blk:(j + 1) * blk], sin_ref[:, j * blk:(j + 1) * blk]
        return jnp.concatenate([u1 * c - u2 * s, u2 * c + u1 * s, jnp.zeros((pad - hd, blk), F32)], axis=0)

    for j in range(4):
        at = slice(j * blk, (j + 1) * blk)
        q_s[:, at] = rotate(0, j).astype(BF16)
        k_s[at, :] = rotate(hd, j).T.astype(BF16)
        v_s[:, at] = qkv_ref[2 * hd:3 * hd, pl.ds(rel(j), blk)]

    base = pl.multiple_of(lax.rem(g, heads_out) * hd, 32)
    for qb in range(4):
        par = qb % 2
        qat = slice(qb * blk, (qb + 1) * blk)
        top = None
        for kb in range(qb + 1):
            kat = slice(kb * blk, (kb + 1) * blk)
            s = jnp.dot(k_s[kat, :], q_s[:, qat], preferred_element_type=F32)
            if kb == qb:
                ki = lax.broadcasted_iota(jnp.int32, (blk, blk), 0)
                qi = lax.broadcasted_iota(jnp.int32, (blk, blk), 1)
                s = jnp.where(ki <= qi, s, -1e30)
            s_s[par, kat, :] = s
            part = jnp.max(s.reshape(blk // 8, 8, blk), axis=0)
            top = part if top is None else jnp.maximum(top, part)
        top = jnp.max(top, axis=0, keepdims=True)
        tot = None
        for kb in range(qb + 1):
            kat = slice(kb * blk, (kb + 1) * blk)
            e = jnp.exp2((s_s[par, kat, :] - top) * (scale * LOG2E))
            s_s[par, kat, :] = e
            part = jnp.sum(e.reshape(blk // 8, 8, blk), axis=0)
            tot = part if tot is None else tot + part
        inv = 1.0 / jnp.sum(tot, axis=0, keepdims=True)
        for kb in range(qb + 1):
            kat = slice(kb * blk, (kb + 1) * blk)
            p_s[par, kat, :] = (s_s[par, kat, :] * inv).astype(BF16)
        nk = (qb + 1) * blk
        ctx = jnp.dot(v_s[:, :nk], p_s[par, :nk, :], preferred_element_type=F32)
        c_s[pl.ds(base, hd), qat] = ctx.astype(BF16)

    @pl.when(lax.rem(g, heads_out) == heads_out - 1)
    def _():
        for j in range(4):
            ctx_ref[pl.ds(rel(j), blk), :] = c_s[:, j * blk:(j + 1) * blk].T


def attention(qkv, cos_tab, sin_tab, tp):
    cols, seq = qkv.shape
    half = cos_tab.shape[0]
    hd = 2 * half
    heads = cols // (3 * hd)
    heads_out = 4
    blk = seq // 4
    tab = pl.BlockSpec((half, seq), lambda g, s: (0, 0))
    return pl.pallas_call(
        functools.partial(attn_kernel, hd ** -0.5, heads_out),
        out_shape=jax.ShapeDtypeStruct((seq, heads * hd), BF16),
        grid_spec=pltpu.PrefetchScalarGridSpec(
            num_scalar_prefetch=1,
            grid=(heads,),
            in_specs=[pl.BlockSpec((3 * hd, seq), lambda g, s: (g, 0)), tab, tab],
            out_specs=pl.BlockSpec((seq, heads_out * hd), lambda g, s: (0, g // heads_out)),
            scratch_shapes=[
                pltpu.VMEM((128, seq), BF16),
                pltpu.VMEM((seq, 128), BF16),
                pltpu.VMEM((hd, seq), BF16),
                pltpu.VMEM((2, seq, blk), F32),
                pltpu.VMEM((2, seq, blk), BF16),
                pltpu.VMEM((heads_out * hd, seq), BF16),
            ],
        ),
        compiler_params=pltpu.CompilerParams(vmem_limit_bytes=VMEM_LIMIT, dimension_semantics=('arbitrary',)),
        cost_estimate=pl.CostEstimate(flops=heads * seq * seq * 2 * 128, bytes_accessed=2 * seq * cols, transcendentals=heads * seq * seq // 2),
        name='attend',
    )(tp, qkv, cos_tab, sin_tab)


def back_kernel(nt, ctx_ref, act_ref, wo_ref, wd_ref, x_ref, out_ref, acc_s, near_s, far_s, recv_s, send_sem, recv_sem):
    p, t = pl.program_id(0), pl.program_id(1)
    tile = jnp.where(lax.rem(p, 2) == 0, t, nt - 1 - t)
    mate, cross = peers()

    def copy(ph, k, src, dev):
        return pltpu.make_async_remote_copy(src_ref=src, dst_ref=recv_s.at[ph, k], send_sem=send_sem.at[ph, k], recv_sem=recv_sem.at[ph, k], device_id={'tp': dev}, device_id_type=pl.DeviceIdType.MESH)

    def near(ph, k):
        return copy(ph, k, near_s.at[lax.rem(k, 3)], mate)

    def far(k):
        return copy(1, k, far_s.at[k], cross)

    @pl.when(jnp.logical_and(p == 0, t == 0))
    def _():
        entry_barrier(mate, cross)

    acc_s[...] = jnp.dot(ctx_ref[...], wo_ref[...], preferred_element_type=F32) + jnp.dot(act_ref[...], wd_ref[...], preferred_element_type=F32)

    @pl.when(p == 0)
    def _():
        @pl.when(t >= 3)
        def _():
            near(0, t - 3).wait_send()

        near_s[lax.rem(t, 3)] = acc_s[...].astype(BF16)
        near(0, t).start()

    @pl.when(p == 1)
    def _():
        near(0, tile).wait_recv()
        far_s[tile] = (acc_s[...] + recv_s[0, tile].astype(F32)).astype(BF16)
        far(tile).start()

    @pl.when(p == 2)
    def _():
        @pl.when(t >= 3)
        def _():
            near(2, t - 3).wait_send()

        @pl.when(t < 3)
        def _():
            near(0, nt - 3 + t).wait_send()

        near_s[lax.rem(t, 3)] = acc_s[...].astype(BF16)
        near(2, t).start()

    @pl.when(p == 3)
    def _():
        near(2, tile).wait_recv()
        far(tile).wait_recv()
        out_ref[...] = (x_ref[...].astype(F32) + acc_s[...] + recv_s[2, tile].astype(F32) + recv_s[1, tile].astype(F32)).astype(BF16)

    @pl.when(jnp.logical_and(p == 3, t == nt - 1))
    def _():
        def drain(k, carry):
            far(k).wait_send()
            return carry

        lax.fori_loop(0, nt, drain, 0)
        for k in range(nt - 3, nt):
            near(2, k).wait_send()


def back(ctx, act, wo, wd, x):
    rows, width = x.shape
    kc, kf = ctx.shape[1], act.shape[1]
    tn = 512
    nt = width // tn

    def tile_at(p, t):
        return 0, jnp.where(lax.rem(p, 2) == 0, t, nt - 1 - t)

    def last_at(p, t):
        return 0, jnp.where(p == 3, nt - 1 - t, nt - 1)

    return pl.pallas_call(
        functools.partial(back_kernel, nt),
        grid=(4, nt),
        out_shape=jax.ShapeDtypeStruct((rows, width), BF16),
        in_specs=[
            pl.BlockSpec((rows, kc), lambda p, t: (3 - p, 0)),
            pl.BlockSpec((rows, kf), lambda p, t: (3 - p, 0)),
            pl.BlockSpec((kc, tn), tile_at),
            pl.BlockSpec((kf, tn), tile_at),
            pl.BlockSpec((rows, tn), last_at),
        ],
        out_specs=pl.BlockSpec((rows, tn), last_at),
        scratch_shapes=[
            pltpu.VMEM((rows, tn), F32),
            pltpu.VMEM((3, rows, tn), BF16),
            pltpu.VMEM((nt, rows, tn), BF16),
            pltpu.VMEM((3, nt, rows, tn), BF16),
            pltpu.SemaphoreType.DMA((3, nt)),
            pltpu.SemaphoreType.DMA((3, nt)),
        ],
        compiler_params=pltpu.CompilerParams(collective_id=1, has_side_effects=True, vmem_limit_bytes=VMEM_LIMIT, dimension_semantics=('arbitrary', 'arbitrary')),
        cost_estimate=pl.CostEstimate(flops=2 * 4 * rows * width * (kc + kf), bytes_accessed=4 * 2 * width * (kc + kf), transcendentals=0),
        name='back',
    )(ctx, act, wo, wd, x)


def solution(mesh):
    def local_layer(hidden_blk, attn_gain, attn_bias, mlp_gain, mlp_bias, w_qkv_part, w_out_part, w_up_part, w_down_part, positions):
        width = hidden_blk.shape[-1]
        x = hidden_blk.reshape(-1, width)
        wq = jnp.transpose(w_qkv_part, (1, 2, 0)).reshape(-1, width)
        half_dim = w_qkv_part.shape[2] // 6
        cos_tab, sin_tab = rotary_tables(positions, half_dim)
        vecs = [v.reshape(1, width) for v in (attn_gain, attn_bias, mlp_gain, mlp_bias)]
        qkv, act = front(x, wq, w_up_part, *vecs)
        tp = lax.axis_index('tp').astype(jnp.int32).reshape(1)
        ctx = attention(qkv, cos_tab, sin_tab, tp)
        out = back(ctx, act, w_out_part, w_down_part, x)
        return out.reshape(hidden_blk.shape)

    return jax.shard_map(local_layer, mesh=mesh, in_specs=(P('dp', 'tp', None), P(), P(), P(), P(), P(None, 'tp', None), P('tp', None), P(None, 'tp'), P('tp', None), P()), out_specs=P('dp', 'tp', None), check_vma=False)
```

```python
import functools

import jax
import jax.numpy as jnp
from jax import lax
from jax.experimental import pallas as pl
from jax.experimental.pallas import tpu as pltpu
from jax.sharding import PartitionSpec as P

F32 = jnp.float32
BF16 = jnp.bfloat16
VMEM_LIMIT = 67_000_000
LOG2E = 1.4426950408889634


def rotary_tables(positions, half_dim):
    inv_freq = 10000.0 ** (-2.0 * jnp.arange(half_dim, dtype=F32) / (2 * half_dim))
    angles = inv_freq[:, None] * positions.astype(F32)[None, :]
    return jnp.cos(angles), jnp.sin(angles)


def peers():
    tp = lax.axis_index('tp')
    mate = tp + 1 - 2 * lax.rem(tp, 2)
    cross = lax.rem(tp + 2, 4)
    return mate, cross


def entry_barrier(mate, cross):
    sem = pltpu.get_barrier_semaphore()
    for dev in (mate, cross):
        pl.semaphore_signal(sem, inc=1, device_id={'tp': dev}, device_id_type=pl.DeviceIdType.MESH)
    pl.semaphore_wait(sem, 2)


def gelu(pre):
    return pre * (lax.erf(pre * (2.0 ** -0.5)) + 1.0) * 0.5


def norm_rows(x_s, a_s, m_s, ga, ba, gm, bm, start, count):
    tall, wide = 16, 512
    width = x_s.shape[1]
    lanes = [slice(j, j + wide) for j in range(0, width, wide)]

    def fold(v):
        return (v[:, 0:128] + v[:, 128:256]) + (v[:, 256:384] + v[:, 384:512])

    for i in range(0, count, tall):
        at = pl.ds(pl.multiple_of(start + i, tall), tall)
        mean = jnp.sum(sum(fold(x_s[at, j].astype(F32)) for j in lanes), axis=-1, keepdims=True) * (1.0 / width)
        tot = 0.0
        for j in lanes:
            c = x_s[at, j].astype(F32) - mean
            tot = tot + fold(c * c)
        inv = lax.rsqrt(jnp.sum(tot, axis=-1, keepdims=True) * (1.0 / width) + 1e-5)
        for j in lanes:
            z = (x_s[at, j].astype(F32) - mean) * inv
            a_s[0, at, j] = (z * ga[:, j] + ba[:, j]).astype(BF16)
            m_s[0, at, j] = (z * gm[:, j] + bm[:, j]).astype(BF16)


def front_kernel(nq, nu, x_hbm, wq_ref, wu_ref, ga, ba, gm, bm, qkv_ref, act_ref, xr, x_s, a_s, m_s, pre_s, load_sem, send_sem, recv_sem, free_sem):
    r, t = pl.program_id(0), pl.program_id(1)
    nt = nq + nu
    here = lax.rem(r, 2)
    even = here == 0
    is_q = jnp.logical_or(jnp.logical_and(even, t < nq), jnp.logical_and(jnp.logical_not(even), t >= nu))
    mate, cross = peers()

    def remote(k):
        if k == 0:
            src, dst, dev = x_hbm, xr, cross
        else:
            buf = a_s if k % 2 else m_s
            src, dst, dev = buf.at[0], buf.at[1], mate
        return pltpu.make_async_remote_copy(src_ref=src, dst_ref=dst, send_sem=send_sem.at[k], recv_sem=recv_sem.at[k], device_id={'tp': dev}, device_id_type=pl.DeviceIdType.MESH)

    def load(src):
        return pltpu.make_async_copy(src, x_s, load_sem)

    def norm():
        load(xr).wait()

        def chunk(i, carry):
            norm_rows(x_s, a_s, m_s, ga, ba, gm, bm, i * 64, 64)
            return carry

        lax.fori_loop(0, x_s.shape[0] // 64, chunk, 0)

    @pl.when(jnp.logical_and(r == 0, t == 0))
    def _():
        load(x_hbm).start()
        entry_barrier(mate, cross)
        remote(0).start()
        norm()
        remote(1).start()
        remote(2).start()

    @pl.when(jnp.logical_and(r == 1, t == 0))
    def _():
        for k in (1, 2):
            remote(k).wait()

    @pl.when(jnp.logical_and(r == 1, t == nt - 2))
    def _():
        remote(0).wait_recv()
        load(xr).start()

    @pl.when(jnp.logical_and(r == 2, t == 0))
    def _():
        pl.semaphore_signal(free_sem, inc=1, device_id={'tp': mate}, device_id_type=pl.DeviceIdType.MESH)
        norm()
        pl.semaphore_wait(free_sem, 1)
        remote(3).start()
        remote(4).start()

    @pl.when(jnp.logical_and(r == 3, t == 0))
    def _():
        for k in (3, 4):
            remote(k).wait()

    @pl.when(is_q)
    def _():
        qkv_ref[...] = lax.dot_general(wq_ref[...], a_s[here], (((1,), (1,)), ((), ())), preferred_element_type=F32).astype(BF16)

    @pl.when(jnp.logical_not(is_q))
    def _():
        for c in range(0, wu_ref.shape[1], 256):
            at = slice(c, c + 256)
            act_ref[:, at] = gelu(pre_s[:, at]).astype(BF16)
            pre_s[:, at] = jnp.dot(m_s[here], wu_ref[:, at], preferred_element_type=F32)

    @pl.when(jnp.logical_and(r == 3, t == nt - 1))
    def _():
        act_ref[...] = gelu(pre_s[...]).astype(BF16)
        remote(0).wait_send()


def front(x, wq, wu, ga, ba, gm, bm):
    rows, width = x.shape
    qcols, ff = wq.shape[0], wu.shape[1]
    tq, tu = 512, 512
    nq, nu = qcols // tq, ff // tu
    nt = nq + nu

    def even(r):
        return lax.rem(r, 2) == 0

    def wq_at(r, t):
        return jnp.where(even(r), jnp.minimum(t, nq - 1), jnp.minimum(nq - 1, nt - 1 - t)), 0

    def wu_at(r, t):
        return 0, jnp.where(even(r), jnp.maximum(t - nq, 0), jnp.maximum(nu - 1 - t, 0))

    def qkv_at(r, t):
        held = jnp.logical_and(jnp.logical_not(even(r)), t < nu)
        return wq_at(r, t)[0], jnp.where(held, r - 1, r)

    def act_at(r, t):
        k = jnp.where(even(r), t - nq, t)
        blk = jnp.where(k <= 0, r - 1, r)
        col = jnp.where(k < 0, nu - 2, jnp.where(k == 0, nu - 1, jnp.minimum(k - 1, nu - 2)))
        col = jnp.where(jnp.logical_and(r == 3, t == nt - 1), nu - 1, col)
        col = jnp.where(blk < 0, 0, col)
        blk = jnp.maximum(blk, 0)
        return blk, jnp.where(even(blk), col, nu - 1 - col)

    vec = pl.BlockSpec((1, width), lambda r, t: (0, 0))
    flops = 2 * 4 * rows * width * (qcols + ff)
    return pl.pallas_call(
        functools.partial(front_kernel, nq, nu),
        grid=(4, nt),
        out_shape=(jax.ShapeDtypeStruct((qcols, 4 * rows), BF16), jax.ShapeDtypeStruct((4 * rows, ff), BF16), jax.ShapeDtypeStruct((rows, width), BF16)),
        in_specs=[pl.BlockSpec(memory_space=pl.ANY), pl.BlockSpec((tq, width), wq_at), pl.BlockSpec((width, tu), wu_at), vec, vec, vec, vec],
        out_specs=(pl.BlockSpec((tq, rows), qkv_at), pl.BlockSpec((rows, tu), act_at), pl.BlockSpec(memory_space=pl.ANY)),
        scratch_shapes=[
            pltpu.VMEM((rows, width), BF16),
            pltpu.VMEM((2, rows, width), BF16),
            pltpu.VMEM((2, rows, width), BF16),
            pltpu.VMEM((rows, tu), F32),
            pltpu.SemaphoreType.DMA,
            pltpu.SemaphoreType.DMA((5,)),
            pltpu.SemaphoreType.DMA((5,)),
            pltpu.SemaphoreType.REGULAR,
        ],
        compiler_params=pltpu.CompilerParams(collective_id=0, has_side_effects=True, vmem_limit_bytes=VMEM_LIMIT, dimension_semantics=('arbitrary', 'arbitrary')),
        cost_estimate=pl.CostEstimate(flops=flops, bytes_accessed=4 * 2 * width * (qcols + ff), transcendentals=0),
        name='front',
    )(x, wq, wu, ga, ba, gm, bm)[:2]


def attn_kernel(scale, heads_out, per_step, tp_ref, qkv_ref, cos_ref, sin_ref, ctx_ref, q_s, k_s, v_s, s_s, p_s, c_s):
    g = pl.program_id(0)
    tp = tp_ref[0]
    half, seq = cos_ref.shape
    hd = 2 * half
    blk = seq // 4
    pad = k_s.shape[2]

    def rel(j):
        return pl.multiple_of((tp ^ j) * blk, blk)

    def rotate(base, j):
        at = pl.ds(rel(j), blk)
        u1 = qkv_ref[base:base + half, at].astype(F32)
        u2 = qkv_ref[base + half:base + hd, at].astype(F32)
        c, s = cos_ref[:, j * blk:(j + 1) * blk], sin_ref[:, j * blk:(j + 1) * blk]
        return jnp.concatenate([u1 * c - u2 * s, u2 * c + u1 * s, jnp.zeros((pad - hd, blk), F32)], axis=0)

    for h in range(per_step):
        for j in range(4):
            at = slice(j * blk, (j + 1) * blk)
            q_s[h, :, at] = rotate(3 * h * hd, j).astype(BF16)
            k_s[h, at, :] = rotate((3 * h + 1) * hd, j).T.astype(BF16)
            v_s[h, :, at] = qkv_ref[(3 * h + 2) * hd:(3 * h + 3) * hd, pl.ds(rel(j), blk)]

    base = pl.multiple_of(lax.rem(g * per_step, heads_out) * hd, 32)
    tops, sums = {}, {}
    order = [(0,0),(0,3),(1,0),(1,3),(0,1),(0,2),(1,2),(1,1)]

    def fold(v, op):
        parts = [v[i:i + 8] for i in range(0, v.shape[0], 8)]
        while len(parts) > 1:
            parts = [op(parts[i], parts[i + 1]) for i in range(0, len(parts), 2)]
        return parts[0]

    def score(u, i):
        h, qb = order[u]
        at = slice(i, i + 128)
        s = jnp.dot(k_s[h, at, :], q_s[h, :, qb * blk:(qb + 1) * blk], preferred_element_type=F32)
        if i >= qb * blk:
            ki = i + lax.broadcasted_iota(jnp.int32, (128, blk), 0)
            qi = qb * blk + lax.broadcasted_iota(jnp.int32, (128, blk), 1)
            s = jnp.where(ki <= qi, s, -1e30)
        s_s[u % 3, at, :] = s
        part = fold(s, jnp.maximum)
        tops[u] = part if i == 0 else jnp.maximum(tops[u], part)

    def weigh(u, i):
        if i == 0:
            tops[u] = jnp.max(tops[u], axis=0, keepdims=True)
        at = slice(i, i + 32)
        e = jnp.exp2((s_s[u % 3, at, :] - tops[u]) * (scale * LOG2E))
        s_s[u % 3, at, :] = e
        part = fold(e, jnp.add)
        sums[u] = part if i == 0 else sums[u] + part

    def mix(u, i):
        if i == 0:
            sums[u] = 1.0 / jnp.sum(sums[u], axis=0, keepdims=True)
        at = slice(i, i + 32)
        p_s[u % 2, at, :] = (s_s[u % 3, at, :] * sums[u]).astype(BF16)

    def finish(u):
        h, qb = order[u]
        nk = (qb + 1) * blk
        ctx = jnp.dot(v_s[h, :, :nk], p_s[u % 2, :nk, :], preferred_element_type=F32)
        c_s[pl.ds(base + h * hd, hd), qb * blk:(qb + 1) * blk] = ctx.astype(BF16)

    def stage(fn, u, tall):
        return [functools.partial(fn, u, i) for i in range(0, (order[u][1] + 1) * blk, tall)]

    def merge(*lists):
        keyed = [((n + 0.5) / len(each), f) for each in lists for n, f in enumerate(each)]
        for _, f in sorted(keyed, key=lambda kf: kf[0]):
            f()

    for n in range(len(order) + 2):
        lists = []
        if 0 <= n - 2:
            lists.append(stage(mix, n - 2, 32))
        if 0 <= n - 1 < len(order):
            lists.append(stage(weigh, n - 1, 32))
        if n < len(order):
            lists.append(stage(score, n, 128))
        merge(*lists)
        if 0 <= n - 2:
            finish(n - 2)

    @pl.when(lax.rem((g + 1) * per_step, heads_out) == 0)
    def _():
        for j in range(4):
            ctx_ref[pl.ds(rel(j), blk), :] = c_s[:, j * blk:(j + 1) * blk].T


def attention(qkv, cos_tab, sin_tab, tp):
    cols, seq = qkv.shape
    half = cos_tab.shape[0]
    hd = 2 * half
    heads = cols // (3 * hd)
    heads_out, per_step = 4, 2
    blk = seq // 4
    tab = pl.BlockSpec((half, seq), lambda g, s: (0, 0))
    return pl.pallas_call(
        functools.partial(attn_kernel, hd ** -0.5, heads_out, per_step),
        out_shape=jax.ShapeDtypeStruct((seq, heads * hd), BF16),
        grid_spec=pltpu.PrefetchScalarGridSpec(
            num_scalar_prefetch=1,
            grid=(heads // per_step,),
            in_specs=[pl.BlockSpec((per_step * 3 * hd, seq), lambda g, s: (g, 0)), tab, tab],
            out_specs=pl.BlockSpec((seq, heads_out * hd), lambda g, s: (0, g * per_step // heads_out)),
            scratch_shapes=[
                pltpu.VMEM((per_step, 128, seq), BF16),
                pltpu.VMEM((per_step, seq, 128), BF16),
                pltpu.VMEM((per_step, hd, seq), BF16),
                pltpu.VMEM((3, seq, blk), F32),
                pltpu.VMEM((2, seq, blk), BF16),
                pltpu.VMEM((heads_out * hd, seq), BF16),
            ],
        ),
        compiler_params=pltpu.CompilerParams(vmem_limit_bytes=VMEM_LIMIT, dimension_semantics=('arbitrary',)),
        cost_estimate=pl.CostEstimate(flops=heads * seq * seq * 2 * 128, bytes_accessed=2 * seq * cols, transcendentals=heads * seq * seq // 2),
        name='attend',
    )(tp, qkv, cos_tab, sin_tab)


def back_kernel(nt, ctx_ref, act_ref, wo_ref, wd_ref, x_ref, out_ref, acc_s, near_s, far_s, recv_s, send_sem, recv_sem):
    p, t = pl.program_id(0), pl.program_id(1)
    tile = jnp.where(lax.rem(p, 2) == 0, t, nt - 1 - t)
    mate, cross = peers()

    def copy(ph, k, src, dev):
        return pltpu.make_async_remote_copy(src_ref=src, dst_ref=recv_s.at[ph, k], send_sem=send_sem.at[ph, k], recv_sem=recv_sem.at[ph, k], device_id={'tp': dev}, device_id_type=pl.DeviceIdType.MESH)

    def near(ph, k):
        return copy(ph, k, near_s.at[lax.rem(k, 3)], mate)

    def far(k):
        return copy(1, k, far_s.at[k], cross)

    @pl.when(jnp.logical_and(p == 0, t == 0))
    def _():
        entry_barrier(mate, cross)

    acc_s[...] = jnp.dot(ctx_ref[...], wo_ref[...], preferred_element_type=F32) + jnp.dot(act_ref[...], wd_ref[...], preferred_element_type=F32)

    @pl.when(p == 0)
    def _():
        @pl.when(t >= 3)
        def _():
            near(0, t - 3).wait_send()

        near_s[lax.rem(t, 3)] = acc_s[...].astype(BF16)
        near(0, t).start()

    @pl.when(p == 1)
    def _():
        near(0, tile).wait_recv()
        far_s[tile] = (acc_s[...] + recv_s[0, tile].astype(F32)).astype(BF16)
        far(tile).start()

    @pl.when(p == 2)
    def _():
        @pl.when(t >= 3)
        def _():
            near(2, t - 3).wait_send()

        @pl.when(t < 3)
        def _():
            near(0, nt - 3 + t).wait_send()

        near_s[lax.rem(t, 3)] = acc_s[...].astype(BF16)
        near(2, t).start()

    @pl.when(p == 3)
    def _():
        near(2, tile).wait_recv()
        far(tile).wait_recv()
        out_ref[...] = (x_ref[...].astype(F32) + acc_s[...] + recv_s[2, tile].astype(F32) + recv_s[1, tile].astype(F32)).astype(BF16)

    @pl.when(jnp.logical_and(p == 3, t == nt - 1))
    def _():
        def drain(k, carry):
            far(k).wait_send()
            return carry

        lax.fori_loop(0, nt, drain, 0)
        for k in range(nt - 3, nt):
            near(2, k).wait_send()


def back(ctx, act, wo, wd, x):
    rows, width = x.shape
    kc, kf = ctx.shape[1], act.shape[1]
    tn = 512
    nt = width // tn

    def tile_at(p, t):
        return 0, jnp.where(lax.rem(p, 2) == 0, t, nt - 1 - t)

    def last_at(p, t):
        return 0, jnp.where(p == 3, nt - 1 - t, nt - 1)

    return pl.pallas_call(
        functools.partial(back_kernel, nt),
        grid=(4, nt),
        out_shape=jax.ShapeDtypeStruct((rows, width), BF16),
        in_specs=[
            pl.BlockSpec((rows, kc), lambda p, t: (3 - p, 0)),
            pl.BlockSpec((rows, kf), lambda p, t: (3 - p, 0)),
            pl.BlockSpec((kc, tn), tile_at),
            pl.BlockSpec((kf, tn), tile_at),
            pl.BlockSpec((rows, tn), last_at),
        ],
        out_specs=pl.BlockSpec((rows, tn), last_at),
        scratch_shapes=[
            pltpu.VMEM((rows, tn), F32),
            pltpu.VMEM((3, rows, tn), BF16),
            pltpu.VMEM((nt, rows, tn), BF16),
            pltpu.VMEM((3, nt, rows, tn), BF16),
            pltpu.SemaphoreType.DMA((3, nt)),
            pltpu.SemaphoreType.DMA((3, nt)),
        ],
        compiler_params=pltpu.CompilerParams(collective_id=1, has_side_effects=True, vmem_limit_bytes=VMEM_LIMIT, dimension_semantics=('arbitrary', 'arbitrary')),
        cost_estimate=pl.CostEstimate(flops=2 * 4 * rows * width * (kc + kf), bytes_accessed=4 * 2 * width * (kc + kf), transcendentals=0),
        name='back',
    )(ctx, act, wo, wd, x)


def solution(mesh):
    def local_layer(hidden_blk, attn_gain, attn_bias, mlp_gain, mlp_bias, w_qkv_part, w_out_part, w_up_part, w_down_part, positions):
        width = hidden_blk.shape[-1]
        x = hidden_blk.reshape(-1, width)
        wq = jnp.transpose(w_qkv_part, (1, 2, 0)).reshape(-1, width)
        half_dim = w_qkv_part.shape[2] // 6
        cos_tab, sin_tab = rotary_tables(positions, half_dim)
        vecs = [v.reshape(1, width) for v in (attn_gain, attn_bias, mlp_gain, mlp_bias)]
        qkv, act = front(x, wq, w_up_part, *vecs)
        tp = lax.axis_index('tp').astype(jnp.int32).reshape(1)
        ctx = attention(qkv, cos_tab, sin_tab, tp)
        out = back(ctx, act, w_out_part, w_down_part, x)
        return out.reshape(hidden_blk.shape)

    return jax.shard_map(local_layer, mesh=mesh, in_specs=(P('dp', 'tp', None), P(), P(), P(), P(), P(None, 'tp', None), P('tp', None), P(None, 'tp'), P('tp', None), P()), out_specs=P('dp', 'tp', None), check_vma=False)
```

```python
import functools

import jax
import jax.numpy as jnp
from jax import lax
from jax.experimental import pallas as pl
from jax.experimental.pallas import tpu as pltpu
from jax.sharding import PartitionSpec as P

F32 = jnp.float32
BF16 = jnp.bfloat16
VMEM_LIMIT = 67_000_000
TALL = 64
LOG2E = 1.4426950408889634


def rotary_tables(positions, half_dim):
    inv_freq = 10000.0 ** (-2.0 * jnp.arange(half_dim, dtype=F32) / (2 * half_dim))
    angles = inv_freq[:, None] * positions.astype(F32)[None, :]
    return jnp.cos(angles), jnp.sin(angles)


def peers():
    tp = lax.axis_index('tp')
    mate = tp + 1 - 2 * lax.rem(tp, 2)
    cross = lax.rem(tp + 2, 4)
    return mate, cross


def entry_barrier(mate, cross):
    sem = pltpu.get_barrier_semaphore()
    for dev in (mate, cross):
        pl.semaphore_signal(sem, inc=1, device_id={'tp': dev}, device_id_type=pl.DeviceIdType.MESH)
    pl.semaphore_wait(sem, 2)


def gelu(pre):
    return pre * (lax.erf(pre * (2.0 ** -0.5)) + 1.0) * 0.5


def norm_rows(x_s, a_s, m_s, ga, ba, gm, bm, start):
    tall, wide = 16, 512
    width = x_s.shape[1]
    lanes = [slice(j, j + wide) for j in range(0, width, wide)]

    def fold(v):
        return (v[:, 0:128] + v[:, 128:256]) + (v[:, 256:384] + v[:, 384:512])

    for i in range(0, TALL, tall):
        at = pl.ds(pl.multiple_of(start + i, tall), tall)
        src = slice(i, i + tall)
        mean = jnp.sum(sum(fold(x_s[src, j].astype(F32)) for j in lanes), axis=-1, keepdims=True) * (1.0 / width)
        tot = 0.0
        for j in lanes:
            c = x_s[src, j].astype(F32) - mean
            tot = tot + fold(c * c)
        inv = lax.rsqrt(jnp.sum(tot, axis=-1, keepdims=True) * (1.0 / width) + 1e-5)
        for j in lanes:
            z = (x_s[src, j].astype(F32) - mean) * inv
            a_s[0, at, j] = (z * ga[:, j] + ba[:, j]).astype(BF16)
            m_s[0, at, j] = (z * gm[:, j] + bm[:, j]).astype(BF16)


def front_kernel(nq, nu, x_hbm, wq_ref, wu_ref, ga_h, ba_h, gm_h, bm_h, qkv_ref, act_ref, xr, x_s, a_s, m_s, pre_s, ga, ba, gm, bm, load_sem, vec_sem, send_sem, recv_sem, free_sem):
    r, t = pl.program_id(0), pl.program_id(1)
    nt = nq + nu
    here = lax.rem(r, 2)
    even = here == 0
    is_q = jnp.logical_or(jnp.logical_and(even, t < nq), jnp.logical_and(jnp.logical_not(even), t >= nu))
    mate, cross = peers()

    def remote(k):
        if k == 0:
            src, dst, dev = x_hbm, xr, cross
        else:
            buf = a_s if k % 2 else m_s
            src, dst, dev = buf.at[0], buf.at[1], mate
        return pltpu.make_async_remote_copy(src_ref=src, dst_ref=dst, send_sem=send_sem.at[k], recv_sem=recv_sem.at[k], device_id={'tp': dev}, device_id_type=pl.DeviceIdType.MESH)

    def norm(src):
        pieces = m_s.shape[1] // TALL

        def load(i):
            k = lax.rem(i, 2)
            return pltpu.make_async_copy(src.at[pl.ds(pl.multiple_of(i * TALL, TALL), TALL), :], x_s.at[k], load_sem.at[k])

        load(0).start()

        def chunk(i, carry):
            @pl.when(i + 1 < pieces)
            def _():
                load(i + 1).start()

            load(i).wait()
            norm_rows(x_s.at[lax.rem(i, 2)], a_s, m_s, ga, ba, gm, bm, i * TALL)
            return carry

        lax.fori_loop(0, pieces, chunk, 0)

    @pl.when(jnp.logical_and(r == 0, t == 0))
    def _():
        vecs = [pltpu.make_async_copy(src, dst, vec_sem.at[k]) for k, (src, dst) in enumerate(((ga_h, ga), (ba_h, ba), (gm_h, gm), (bm_h, bm)))]
        for each in vecs:
            each.start()
        entry_barrier(mate, cross)
        remote(0).start()
        for each in vecs:
            each.wait()
        norm(x_hbm)
        remote(1).start()
        remote(2).start()

    @pl.when(jnp.logical_and(r == 1, t == 0))
    def _():
        for k in (1, 2):
            remote(k).wait()

    @pl.when(jnp.logical_and(r == 2, t == 0))
    def _():
        pl.semaphore_signal(free_sem, inc=1, device_id={'tp': mate}, device_id_type=pl.DeviceIdType.MESH)
        remote(0).wait_recv()
        norm(xr)
        pl.semaphore_wait(free_sem, 1)
        remote(3).start()
        remote(4).start()

    @pl.when(jnp.logical_and(r == 3, t == 0))
    def _():
        for k in (3, 4):
            remote(k).wait()

    @pl.when(is_q)
    def _():
        for c in range(0, wq_ref.shape[0], 256):
            at = slice(c, c + 256)
            qkv_ref[at, :] = lax.dot_general(wq_ref[at, :], a_s[here], (((1,), (1,)), ((), ())), preferred_element_type=F32).astype(BF16)

    @pl.when(jnp.logical_not(is_q))
    def _():
        for c in range(0, wu_ref.shape[1], 256):
            at = slice(c, c + 256)
            act_ref[:, at] = gelu(pre_s[:, at]).astype(BF16)
            pre_s[:, at] = jnp.dot(m_s[here], wu_ref[:, at], preferred_element_type=F32)

    @pl.when(jnp.logical_and(r == 3, t == nt - 1))
    def _():
        for c in range(0, wu_ref.shape[1], 256):
            at = slice(c, c + 256)
            act_ref[:, at] = gelu(pre_s[:, at]).astype(BF16)
        remote(0).wait_send()


def front(x, wq, wu, ga, ba, gm, bm):
    rows, width = x.shape
    qcols, ff = wq.shape[0], wu.shape[1]
    tq, tu = 512, 768
    nq, nu = qcols // tq, ff // tu
    nt = nq + nu

    def even(r):
        return lax.rem(r, 2) == 0

    def wq_at(r, t):
        return jnp.where(even(r), jnp.minimum(t, nq - 1), jnp.minimum(nq - 1, nt - 1 - t)), 0

    def wu_at(r, t):
        return 0, jnp.where(even(r), jnp.maximum(t - nq, 0), jnp.maximum(nu - 1 - t, 0))

    def qkv_at(r, t):
        held = jnp.logical_and(jnp.logical_not(even(r)), t < nu)
        return wq_at(r, t)[0], jnp.where(held, r - 1, r)

    def act_at(r, t):
        k = jnp.where(even(r), t - nq, t)
        blk = jnp.where(k <= 0, r - 1, r)
        col = jnp.where(k < 0, nu - 2, jnp.where(k == 0, nu - 1, jnp.minimum(k - 1, nu - 2)))
        col = jnp.where(jnp.logical_and(r == 3, t == nt - 1), nu - 1, col)
        col = jnp.where(blk < 0, 0, col)
        blk = jnp.maximum(blk, 0)
        return blk, jnp.where(even(blk), col, nu - 1 - col)

    flops = 2 * 4 * rows * width * (qcols + ff)
    return pl.pallas_call(
        functools.partial(front_kernel, nq, nu),
        grid=(4, nt),
        out_shape=(jax.ShapeDtypeStruct((qcols, 4 * rows), BF16), jax.ShapeDtypeStruct((4 * rows, ff), BF16), jax.ShapeDtypeStruct((rows, width), BF16)),
        in_specs=[pl.BlockSpec(memory_space=pl.ANY), pl.BlockSpec((tq, width), wq_at), pl.BlockSpec((width, tu), wu_at)] + [pl.BlockSpec(memory_space=pl.ANY)] * 4,
        out_specs=(pl.BlockSpec((tq, rows), qkv_at), pl.BlockSpec((rows, tu), act_at), pl.BlockSpec(memory_space=pl.ANY)),
        scratch_shapes=[
            pltpu.VMEM((2, TALL, width), BF16),
            pltpu.VMEM((2, rows, width), BF16),
            pltpu.VMEM((2, rows, width), BF16),
            pltpu.VMEM((rows, tu), F32),
            pltpu.VMEM((1, width), F32),
            pltpu.VMEM((1, width), F32),
            pltpu.VMEM((1, width), F32),
            pltpu.VMEM((1, width), F32),
            pltpu.SemaphoreType.DMA((2,)),
            pltpu.SemaphoreType.DMA((4,)),
            pltpu.SemaphoreType.DMA((5,)),
            pltpu.SemaphoreType.DMA((5,)),
            pltpu.SemaphoreType.REGULAR,
        ],
        compiler_params=pltpu.CompilerParams(collective_id=0, has_side_effects=True, vmem_limit_bytes=VMEM_LIMIT, dimension_semantics=('arbitrary', 'arbitrary')),
        cost_estimate=pl.CostEstimate(flops=flops, bytes_accessed=4 * 2 * width * (qcols + ff), transcendentals=0),
        name='front',
    )(x, wq, wu, ga, ba, gm, bm)[:2]


def attn_kernel(scale, heads_out, per_step, tp_ref, qkv_ref, cos_ref, sin_ref, ctx_ref, q_s, k_s, v_s, s_s, p_s, c_s):
    g = pl.program_id(0)
    tp = tp_ref[0]
    half, seq = cos_ref.shape
    hd = 2 * half
    blk = seq // 4
    pad = k_s.shape[2]

    def rel(j):
        return pl.multiple_of((tp ^ j) * blk, blk)

    def rotate(base, j):
        at = pl.ds(rel(j), blk)
        u1 = qkv_ref[base:base + half, at].astype(F32)
        u2 = qkv_ref[base + half:base + hd, at].astype(F32)
        c, s = cos_ref[:, j * blk:(j + 1) * blk], sin_ref[:, j * blk:(j + 1) * blk]
        return jnp.concatenate([u1 * c - u2 * s, u2 * c + u1 * s, jnp.zeros((pad - hd, blk), F32)], axis=0)

    for h in range(per_step):
        for j in range(4):
            at = slice(j * blk, (j + 1) * blk)
            q_s[h, :, at] = rotate(3 * h * hd, j).astype(BF16)
            k_s[h, at, :] = rotate((3 * h + 1) * hd, j).T.astype(BF16)
            v_s[h, :, at] = qkv_ref[(3 * h + 2) * hd:(3 * h + 3) * hd, pl.ds(rel(j), blk)]

    base = pl.multiple_of(lax.rem(g * per_step, heads_out) * hd, 32)
    tops, sums = {}, {}
    order = [(0,0),(0,3),(1,0),(1,3),(0,1),(0,2),(1,2),(1,1)]

    def fold(v, op):
        parts = [v[i:i + 8] for i in range(0, v.shape[0], 8)]
        while len(parts) > 1:
            parts = [op(parts[i], parts[i + 1]) for i in range(0, len(parts), 2)]
        return parts[0]

    def score(u, i):
        h, qb = order[u]
        at = slice(i, i + 128)
        s = jnp.dot(k_s[h, at, :], q_s[h, :, qb * blk:(qb + 1) * blk], preferred_element_type=F32)
        if i >= qb * blk:
            ki = i + lax.broadcasted_iota(jnp.int32, (128, blk), 0)
            qi = qb * blk + lax.broadcasted_iota(jnp.int32, (128, blk), 1)
            s = jnp.where(ki <= qi, s, -1e30)
        s_s[u % 3, at, :] = s
        part = fold(s, jnp.maximum)
        tops[u] = part if i == 0 else jnp.maximum(tops[u], part)

    def weigh(u, i):
        if i == 0:
            tops[u] = jnp.max(tops[u], axis=0, keepdims=True)
        at = slice(i, i + 32)
        e = jnp.exp2((s_s[u % 3, at, :] - tops[u]) * (scale * LOG2E))
        s_s[u % 3, at, :] = e
        part = fold(e, jnp.add)
        sums[u] = part if i == 0 else sums[u] + part

    def mix(u, i):
        if i == 0:
            sums[u] = 1.0 / jnp.sum(sums[u], axis=0, keepdims=True)
        at = slice(i, i + 32)
        p_s[u % 2, at, :] = (s_s[u % 3, at, :] * sums[u]).astype(BF16)

    def finish(u):
        h, qb = order[u]
        nk = (qb + 1) * blk
        ctx = jnp.dot(v_s[h, :, :nk], p_s[u % 2, :nk, :], preferred_element_type=F32)
        c_s[pl.ds(base + h * hd, hd), qb * blk:(qb + 1) * blk] = ctx.astype(BF16)

    def stage(fn, u, tall):
        return [functools.partial(fn, u, i) for i in range(0, (order[u][1] + 1) * blk, tall)]

    def merge(*lists):
        keyed = [((n + 0.5) / len(each), f) for each in lists for n, f in enumerate(each)]
        for _, f in sorted(keyed, key=lambda kf: kf[0]):
            f()

    for n in range(len(order) + 2):
        lists = []
        if 0 <= n - 2:
            lists.append(stage(mix, n - 2, 32))
        if 0 <= n - 1 < len(order):
            lists.append(stage(weigh, n - 1, 32))
        if n < len(order):
            lists.append(stage(score, n, 128))
        merge(*lists)
        if 0 <= n - 2:
            finish(n - 2)

    @pl.when(lax.rem((g + 1) * per_step, heads_out) == 0)
    def _():
        for j in range(4):
            ctx_ref[pl.ds(rel(j), blk), :] = c_s[:, j * blk:(j + 1) * blk].T


def attention(qkv, cos_tab, sin_tab, tp):
    cols, seq = qkv.shape
    half = cos_tab.shape[0]
    hd = 2 * half
    heads = cols // (3 * hd)
    heads_out, per_step = 4, 2
    blk = seq // 4
    tab = pl.BlockSpec((half, seq), lambda g, s: (0, 0))
    return pl.pallas_call(
        functools.partial(attn_kernel, hd ** -0.5, heads_out, per_step),
        out_shape=jax.ShapeDtypeStruct((seq, heads * hd), BF16),
        grid_spec=pltpu.PrefetchScalarGridSpec(
            num_scalar_prefetch=1,
            grid=(heads // per_step,),
            in_specs=[pl.BlockSpec((per_step * 3 * hd, seq), lambda g, s: (g, 0)), tab, tab],
            out_specs=pl.BlockSpec((seq, heads_out * hd), lambda g, s: (0, g * per_step // heads_out)),
            scratch_shapes=[
                pltpu.VMEM((per_step, 128, seq), BF16),
                pltpu.VMEM((per_step, seq, 128), BF16),
                pltpu.VMEM((per_step, hd, seq), BF16),
                pltpu.VMEM((3, seq, blk), F32),
                pltpu.VMEM((2, seq, blk), BF16),
                pltpu.VMEM((heads_out * hd, seq), BF16),
            ],
        ),
        compiler_params=pltpu.CompilerParams(vmem_limit_bytes=VMEM_LIMIT, dimension_semantics=('arbitrary',)),
        cost_estimate=pl.CostEstimate(flops=heads * seq * seq * 2 * 128, bytes_accessed=2 * seq * cols, transcendentals=heads * seq * seq // 2),
        name='attend',
    )(tp, qkv, cos_tab, sin_tab)


def back_kernel(nt, ctx_ref, act_ref, wo_ref, wd_ref, x_ref, out_ref, acc_s, near_s, recv_s, send_sem, recv_sem):
    p, t = pl.program_id(0), pl.program_id(1)
    tile = jnp.where(lax.rem(p, 2) == 0, t, nt - 1 - t)
    mate, cross = peers()

    def copy(ph, k, src, dev):
        return pltpu.make_async_remote_copy(src_ref=src, dst_ref=recv_s.at[ph, k], send_sem=send_sem.at[ph, k], recv_sem=recv_sem.at[ph, k], device_id={'tp': dev}, device_id_type=pl.DeviceIdType.MESH)

    def by_rows(add):
        def chunk(i, carry):
            add(pl.ds(pl.multiple_of(i * 64, 64), 64))
            return carry

        lax.fori_loop(0, acc_s.shape[0] // 64, chunk, 0)

    def near(ph, k):
        return copy(ph, k, near_s.at[lax.rem(k, 3)], mate)

    def far(k):
        return copy(1, k, recv_s.at[0, k], cross)

    @pl.when(jnp.logical_and(p == 0, t == 0))
    def _():
        entry_barrier(mate, cross)

    for c in range(0, acc_s.shape[1], 256):
        at = slice(c, c + 256)
        acc_s[:, at] = jnp.dot(ctx_ref[...], wo_ref[:, at], preferred_element_type=F32) + jnp.dot(act_ref[...], wd_ref[:, at], preferred_element_type=F32)

    @pl.when(p == 0)
    def _():
        @pl.when(t >= 3)
        def _():
            near(0, t - 3).wait_send()

        near_s[lax.rem(t, 3)] = acc_s[...].astype(BF16)
        near(0, t).start()

    @pl.when(p == 1)
    def _():
        near(0, tile).wait_recv()

        def add(at):
            recv_s[0, tile, at, :] = (acc_s[at, :] + recv_s[0, tile, at, :].astype(F32)).astype(BF16)

        by_rows(add)
        far(tile).start()

    @pl.when(p == 2)
    def _():
        @pl.when(t >= 3)
        def _():
            near(2, t - 3).wait_send()

        @pl.when(t == 0)
        def _():
            for k in range(nt - 3, nt):
                near(0, k).wait_send()

        near_s[lax.rem(t, 3)] = acc_s[...].astype(BF16)
        near(2, t).start()

    @pl.when(p == 3)
    def _():
        near(2, tile).wait_recv()
        far(tile).wait_recv()

        def add(at):
            out_ref[at, :] = (x_ref[at, :].astype(F32) + acc_s[at, :] + recv_s[2, tile, at, :].astype(F32) + recv_s[1, tile, at, :].astype(F32)).astype(BF16)

        by_rows(add)

    @pl.when(jnp.logical_and(p == 3, t == nt - 1))
    def _():
        def drain(k, carry):
            far(k).wait_send()
            return carry

        lax.fori_loop(0, nt, drain, 0)
        for k in range(nt - 3, nt):
            near(2, k).wait_send()


def back(ctx, act, wo, wd, x):
    rows, width = x.shape
    kc, kf = ctx.shape[1], act.shape[1]
    tn = 768
    nt = width // tn

    def tile_at(p, t):
        return 0, jnp.where(lax.rem(p, 2) == 0, t, nt - 1 - t)

    def last_at(p, t):
        return 0, jnp.where(p == 3, nt - 1 - t, nt - 1)

    return pl.pallas_call(
        functools.partial(back_kernel, nt),
        grid=(4, nt),
        out_shape=jax.ShapeDtypeStruct((rows, width), BF16),
        in_specs=[
            pl.BlockSpec((rows, kc), lambda p, t: (3 - p, 0)),
            pl.BlockSpec((rows, kf), lambda p, t: (3 - p, 0)),
            pl.BlockSpec((kc, tn), tile_at),
            pl.BlockSpec((kf, tn), tile_at),
            pl.BlockSpec((rows, tn), last_at),
        ],
        out_specs=pl.BlockSpec((rows, tn), last_at),
        scratch_shapes=[
            pltpu.VMEM((rows, tn), F32),
            pltpu.VMEM((3, rows, tn), BF16),
            pltpu.VMEM((3, nt, rows, tn), BF16),
            pltpu.SemaphoreType.DMA((3, nt)),
            pltpu.SemaphoreType.DMA((3, nt)),
        ],
        compiler_params=pltpu.CompilerParams(collective_id=1, has_side_effects=True, vmem_limit_bytes=VMEM_LIMIT, dimension_semantics=('arbitrary', 'arbitrary')),
        cost_estimate=pl.CostEstimate(flops=2 * 4 * rows * width * (kc + kf), bytes_accessed=4 * 2 * width * (kc + kf), transcendentals=0),
        name='back',
    )(ctx, act, wo, wd, x)


def solution(mesh):
    def local_layer(hidden_blk, attn_gain, attn_bias, mlp_gain, mlp_bias, w_qkv_part, w_out_part, w_up_part, w_down_part, positions):
        width = hidden_blk.shape[-1]
        x = hidden_blk.reshape(-1, width)
        wq = jnp.transpose(w_qkv_part, (1, 2, 0)).reshape(-1, width)
        half_dim = w_qkv_part.shape[2] // 6
        cos_tab, sin_tab = rotary_tables(positions, half_dim)
        vecs = [v.reshape(1, width) for v in (attn_gain, attn_bias, mlp_gain, mlp_bias)]
        qkv, act = front(x, wq, w_up_part, *vecs)
        tp = lax.axis_index('tp').astype(jnp.int32).reshape(1)
        ctx = attention(qkv, cos_tab, sin_tab, tp)
        out = back(ctx, act, w_out_part, w_down_part, x)
        return out.reshape(hidden_blk.shape)

    return jax.shard_map(local_layer, mesh=mesh, in_specs=(P('dp', 'tp', None), P(), P(), P(), P(), P(None, 'tp', None), P('tp', None), P(None, 'tp'), P('tp', None), P()), out_specs=P('dp', 'tp', None), check_vma=False)
```

```python
import functools

import jax
import jax.numpy as jnp
from jax import lax
from jax.experimental import pallas as pl
from jax.experimental.pallas import tpu as pltpu
from jax.sharding import PartitionSpec as P

F32 = jnp.float32
BF16 = jnp.bfloat16
VMEM_LIMIT = 67_000_000
TALL = 64
LOG2E = 1.4426950408889634


def rotary_tables(positions, half_dim):
    inv_freq = 10000.0 ** (-2.0 * jnp.arange(half_dim, dtype=F32) / (2 * half_dim))
    angles = inv_freq[:, None] * positions.astype(F32)[None, :]
    return jnp.cos(angles), jnp.sin(angles)


def peers():
    tp = lax.axis_index('tp')
    mate = tp + 1 - 2 * lax.rem(tp, 2)
    cross = lax.rem(tp + 2, 4)
    return mate, cross


def entry_barrier(mate, cross):
    sem = pltpu.get_barrier_semaphore()
    for dev in (mate, cross):
        pl.semaphore_signal(sem, inc=1, device_id={'tp': dev}, device_id_type=pl.DeviceIdType.MESH)
    pl.semaphore_wait(sem, 2)


def gelu(pre):
    return pre * (lax.erf(pre * (2.0 ** -0.5)) + 1.0) * 0.5


def norm_rows(x_s, a_s, m_s, ga, ba, gm, bm, start):
    tall, wide = 16, 512
    width = x_s.shape[1]
    lanes = [slice(j, j + wide) for j in range(0, width, wide)]

    def fold(v):
        return (v[:, 0:128] + v[:, 128:256]) + (v[:, 256:384] + v[:, 384:512])

    for i in range(0, TALL, tall):
        at = pl.ds(pl.multiple_of(start + i, tall), tall)
        src = slice(i, i + tall)
        mean = jnp.sum(sum(fold(x_s[src, j].astype(F32)) for j in lanes), axis=-1, keepdims=True) * (1.0 / width)
        tot = 0.0
        for j in lanes:
            c = x_s[src, j].astype(F32) - mean
            tot = tot + fold(c * c)
        inv = lax.rsqrt(jnp.sum(tot, axis=-1, keepdims=True) * (1.0 / width) + 1e-5)
        for j in lanes:
            z = (x_s[src, j].astype(F32) - mean) * inv
            a_s[0, at, j] = (z * ga[:, j] + ba[:, j]).astype(BF16)
            m_s[0, at, j] = (z * gm[:, j] + bm[:, j]).astype(BF16)


def front_kernel(nq, nu, x_hbm, wq_ref, wu_ref, ga_h, ba_h, gm_h, bm_h, qkv_ref, act_ref, xr, x_s, a_s, m_s, pre_s, ga, ba, gm, bm, load_sem, vec_sem, send_sem, recv_sem, free_sem):
    r, t = pl.program_id(0), pl.program_id(1)
    nt = nq + nu
    here = lax.rem(r, 2)
    even = here == 0
    is_q = jnp.logical_or(jnp.logical_and(even, t < nq), jnp.logical_and(jnp.logical_not(even), t >= nu))
    mate, cross = peers()

    def remote(k):
        if k == 0:
            src, dst, dev = x_hbm, xr, cross
        else:
            buf = a_s if k % 2 else m_s
            src, dst, dev = buf.at[0], buf.at[1], mate
        return pltpu.make_async_remote_copy(src_ref=src, dst_ref=dst, send_sem=send_sem.at[k], recv_sem=recv_sem.at[k], device_id={'tp': dev}, device_id_type=pl.DeviceIdType.MESH)

    def norm(src):
        pieces = m_s.shape[1] // TALL

        def load(i):
            k = lax.rem(i, 2)
            return pltpu.make_async_copy(src.at[pl.ds(pl.multiple_of(i * TALL, TALL), TALL), :], x_s.at[k], load_sem.at[k])

        load(0).start()

        def chunk(i, carry):
            @pl.when(i + 1 < pieces)
            def _():
                load(i + 1).start()

            load(i).wait()
            norm_rows(x_s.at[lax.rem(i, 2)], a_s, m_s, ga, ba, gm, bm, i * TALL)
            return carry

        lax.fori_loop(0, pieces, chunk, 0)

    @pl.when(jnp.logical_and(r == 0, t == 0))
    def _():
        vecs = [pltpu.make_async_copy(src, dst, vec_sem.at[k]) for k, (src, dst) in enumerate(((ga_h, ga), (ba_h, ba), (gm_h, gm), (bm_h, bm)))]
        for each in vecs:
            each.start()
        entry_barrier(mate, cross)
        remote(0).start()
        for each in vecs:
            each.wait()
        norm(x_hbm)
        remote(1).start()
        remote(2).start()

    @pl.when(jnp.logical_and(r == 1, t == 0))
    def _():
        for k in (1, 2):
            remote(k).wait()

    @pl.when(jnp.logical_and(r == 2, t == 0))
    def _():
        pl.semaphore_signal(free_sem, inc=1, device_id={'tp': mate}, device_id_type=pl.DeviceIdType.MESH)
        remote(0).wait_recv()
        norm(xr)
        pl.semaphore_wait(free_sem, 1)
        remote(3).start()
        remote(4).start()

    @pl.when(jnp.logical_and(r == 3, t == 0))
    def _():
        for k in (3, 4):
            remote(k).wait()

    @pl.when(is_q)
    def _():
        for c in range(0, wq_ref.shape[0], 256):
            at = slice(c, c + 256)
            qkv_ref[at, :] = lax.dot_general(wq_ref[at, :], a_s[here], (((1,), (1,)), ((), ())), preferred_element_type=F32).astype(BF16)

    @pl.when(jnp.logical_not(is_q))
    def _():
        for c in range(0, wu_ref.shape[1], 256):
            at = slice(c, c + 256)
            act_ref[:, at] = gelu(pre_s[:, at]).astype(BF16)
            pre_s[:, at] = jnp.dot(m_s[here], wu_ref[:, at], preferred_element_type=F32)

    @pl.when(jnp.logical_and(r == 3, t == nt - 1))
    def _():
        for c in range(0, wu_ref.shape[1], 256):
            at = slice(c, c + 256)
            act_ref[:, at] = gelu(pre_s[:, at]).astype(BF16)
        remote(0).wait_send()


def front(x, wq, wu, ga, ba, gm, bm):
    rows, width = x.shape
    qcols, ff = wq.shape[0], wu.shape[1]
    tq, tu = 512, 768
    nq, nu = qcols // tq, ff // tu
    nt = nq + nu

    def even(r):
        return lax.rem(r, 2) == 0

    def wq_at(r, t):
        return jnp.where(even(r), jnp.minimum(t, nq - 1), jnp.minimum(nq - 1, nt - 1 - t)), 0

    def wu_at(r, t):
        return 0, jnp.where(even(r), jnp.maximum(t - nq, 0), jnp.maximum(nu - 1 - t, 0))

    def qkv_at(r, t):
        held = jnp.logical_and(jnp.logical_not(even(r)), t < nu)
        return wq_at(r, t)[0], jnp.where(held, r - 1, r)

    def act_at(r, t):
        k = jnp.where(even(r), t - nq, t)
        blk = jnp.where(k <= 0, r - 1, r)
        col = jnp.where(k < 0, nu - 2, jnp.where(k == 0, nu - 1, jnp.minimum(k - 1, nu - 2)))
        col = jnp.where(jnp.logical_and(r == 3, t == nt - 1), nu - 1, col)
        col = jnp.where(blk < 0, 0, col)
        blk = jnp.maximum(blk, 0)
        return blk, jnp.where(even(blk), col, nu - 1 - col)

    flops = 2 * 4 * rows * width * (qcols + ff)
    return pl.pallas_call(
        functools.partial(front_kernel, nq, nu),
        grid=(4, nt),
        out_shape=(jax.ShapeDtypeStruct((qcols, 4 * rows), BF16), jax.ShapeDtypeStruct((4 * rows, ff), BF16), jax.ShapeDtypeStruct((rows, width), BF16)),
        in_specs=[pl.BlockSpec(memory_space=pl.ANY), pl.BlockSpec((tq, width), wq_at), pl.BlockSpec((width, tu), wu_at)] + [pl.BlockSpec(memory_space=pl.ANY)] * 4,
        out_specs=(pl.BlockSpec((tq, rows), qkv_at), pl.BlockSpec((rows, tu), act_at), pl.BlockSpec(memory_space=pl.ANY)),
        scratch_shapes=[
            pltpu.VMEM((2, TALL, width), BF16),
            pltpu.VMEM((2, rows, width), BF16),
            pltpu.VMEM((2, rows, width), BF16),
            pltpu.VMEM((rows, tu), F32),
            pltpu.VMEM((1, width), F32),
            pltpu.VMEM((1, width), F32),
            pltpu.VMEM((1, width), F32),
            pltpu.VMEM((1, width), F32),
            pltpu.SemaphoreType.DMA((2,)),
            pltpu.SemaphoreType.DMA((4,)),
            pltpu.SemaphoreType.DMA((5,)),
            pltpu.SemaphoreType.DMA((5,)),
            pltpu.SemaphoreType.REGULAR,
        ],
        compiler_params=pltpu.CompilerParams(collective_id=0, has_side_effects=True, vmem_limit_bytes=VMEM_LIMIT, dimension_semantics=('arbitrary', 'arbitrary')),
        cost_estimate=pl.CostEstimate(flops=flops, bytes_accessed=4 * 2 * width * (qcols + ff), transcendentals=0),
        name='front',
    )(x, wq, wu, ga, ba, gm, bm)[:2]


def attn_kernel(scale, heads_out, per_step, tp_ref, qkv_ref, cos_ref, sin_ref, ctx_ref, q_s, k_s, v_s, s_s, p_s, c_s):
    g = pl.program_id(0)
    tp = tp_ref[0]
    half, seq = cos_ref.shape
    hd = 2 * half
    blk = seq // 4
    pad = k_s.shape[2]

    def rel(j):
        return pl.multiple_of((tp ^ j) * blk, blk)

    def rotate(base, j):
        at = pl.ds(rel(j), blk)
        u1 = qkv_ref[base:base + half, at].astype(F32)
        u2 = qkv_ref[base + half:base + hd, at].astype(F32)
        c, s = cos_ref[:, j * blk:(j + 1) * blk], sin_ref[:, j * blk:(j + 1) * blk]
        return jnp.concatenate([u1 * c - u2 * s, u2 * c + u1 * s, jnp.zeros((pad - hd, blk), F32)], axis=0)

    for h in range(per_step):
        for j in range(4):
            at = slice(j * blk, (j + 1) * blk)
            q_s[h, :, at] = rotate(3 * h * hd, j).astype(BF16)
            k_s[h, at, :] = rotate((3 * h + 1) * hd, j).T.astype(BF16)
            v_s[h, :, at] = qkv_ref[(3 * h + 2) * hd:(3 * h + 3) * hd, pl.ds(rel(j), blk)]

    base = pl.multiple_of(lax.rem(g * per_step, heads_out) * hd, 32)
    tops, sums = {}, {}
    order = [(0,0),(0,3),(1,0),(1,3),(0,1),(0,2),(1,2),(1,1)]

    def fold(v, op):
        parts = [v[i:i + 8] for i in range(0, v.shape[0], 8)]
        while len(parts) > 1:
            parts = [op(parts[i], parts[i + 1]) for i in range(0, len(parts), 2)]
        return parts[0]

    def score(u, i):
        h, qb = order[u]
        at = slice(i, i + 128)
        s = jnp.dot(k_s[h, at, :], q_s[h, :, qb * blk:(qb + 1) * blk], preferred_element_type=F32)
        if i >= qb * blk:
            ki = i + lax.broadcasted_iota(jnp.int32, (128, blk), 0)
            qi = qb * blk + lax.broadcasted_iota(jnp.int32, (128, blk), 1)
            s = jnp.where(ki <= qi, s, -1e30)
        s_s[u % 3, at, :] = s
        part = fold(s, jnp.maximum)
        tops[u] = part if i == 0 else jnp.maximum(tops[u], part)

    def weigh(u, i):
        if i == 0:
            tops[u] = jnp.max(tops[u], axis=0, keepdims=True)
        at = slice(i, i + 32)
        e = jnp.exp2((s_s[u % 3, at, :] - tops[u]) * (scale * LOG2E))
        s_s[u % 3, at, :] = e
        part = fold(e, jnp.add)
        sums[u] = part if i == 0 else sums[u] + part

    def mix(u, i):
        if i == 0:
            sums[u] = 1.0 / jnp.sum(sums[u], axis=0, keepdims=True)
        at = slice(i, i + 32)
        p_s[u % 2, at, :] = (s_s[u % 3, at, :] * sums[u]).astype(BF16)

    def finish(u):
        h, qb = order[u]
        nk = (qb + 1) * blk
        ctx = jnp.dot(v_s[h, :, :nk], p_s[u % 2, :nk, :], preferred_element_type=F32)
        c_s[pl.ds(base + h * hd, hd), qb * blk:(qb + 1) * blk] = ctx.astype(BF16)

    def stage(fn, u, tall):
        return [functools.partial(fn, u, i) for i in range(0, (order[u][1] + 1) * blk, tall)]

    def merge(*lists):
        keyed = [((n + 0.5) / len(each), f) for each in lists for n, f in enumerate(each)]
        for _, f in sorted(keyed, key=lambda kf: kf[0]):
            f()

    for n in range(len(order) + 2):
        lists = []
        if 0 <= n - 2:
            lists.append(stage(mix, n - 2, 32))
        if 0 <= n - 1 < len(order):
            lists.append(stage(weigh, n - 1, 32))
        if n < len(order):
            lists.append(stage(score, n, 128))
        merge(*lists)
        if 0 <= n - 2:
            finish(n - 2)

    @pl.when(lax.rem((g + 1) * per_step, heads_out) == 0)
    def _():
        for j in range(4):
            ctx_ref[pl.ds(rel(j), blk), :] = c_s[:, j * blk:(j + 1) * blk].T


def attention(qkv, cos_tab, sin_tab, tp):
    cols, seq = qkv.shape
    half = cos_tab.shape[0]
    hd = 2 * half
    heads = cols // (3 * hd)
    heads_out, per_step = 4, 2
    blk = seq // 4
    tab = pl.BlockSpec((half, seq), lambda g, s: (0, 0))
    return pl.pallas_call(
        functools.partial(attn_kernel, hd ** -0.5, heads_out, per_step),
        out_shape=jax.ShapeDtypeStruct((seq, heads * hd), BF16),
        grid_spec=pltpu.PrefetchScalarGridSpec(
            num_scalar_prefetch=1,
            grid=(heads // per_step,),
            in_specs=[pl.BlockSpec((per_step * 3 * hd, seq), lambda g, s: (g, 0)), tab, tab],
            out_specs=pl.BlockSpec((seq, heads_out * hd), lambda g, s: (0, g * per_step // heads_out)),
            scratch_shapes=[
                pltpu.VMEM((per_step, 128, seq), BF16),
                pltpu.VMEM((per_step, seq, 128), BF16),
                pltpu.VMEM((per_step, hd, seq), BF16),
                pltpu.VMEM((3, seq, blk), F32),
                pltpu.VMEM((2, seq, blk), BF16),
                pltpu.VMEM((heads_out * hd, seq), BF16),
            ],
        ),
        compiler_params=pltpu.CompilerParams(vmem_limit_bytes=VMEM_LIMIT, dimension_semantics=('arbitrary',)),
        cost_estimate=pl.CostEstimate(flops=heads * seq * seq * 2 * 128, bytes_accessed=2 * seq * cols, transcendentals=heads * seq * seq // 2),
        name='attend',
    )(tp, qkv, cos_tab, sin_tab)


def back_kernel(nt, ctx_ref, act_ref, wo_ref, wd_ref, x_ref, out_ref, acc_s, near_s, recv_s, send_sem, recv_sem):
    p, t = pl.program_id(0), pl.program_id(1)
    tile = jnp.where(lax.rem(p, 2) == 0, t, nt - 1 - t)
    mate, cross = peers()

    def copy(ph, k, src, dev):
        return pltpu.make_async_remote_copy(src_ref=src, dst_ref=recv_s.at[ph, k], send_sem=send_sem.at[ph, k], recv_sem=recv_sem.at[ph, k], device_id={'tp': dev}, device_id_type=pl.DeviceIdType.MESH)

    def by_rows(add):
        def chunk(i, carry):
            add(pl.ds(pl.multiple_of(i * 64, 64), 64))
            return carry

        lax.fori_loop(0, acc_s.shape[0] // 64, chunk, 0, unroll=2)

    def near(ph, k):
        return copy(ph, k, near_s.at[lax.rem(k, 3)], mate)

    def far(k):
        return copy(1, k, recv_s.at[0, k], cross)

    @pl.when(jnp.logical_and(p == 0, t == 0))
    def _():
        entry_barrier(mate, cross)

    for c in range(0, acc_s.shape[1], 256):
        at = slice(c, c + 256)
        acc_s[:, at] = jnp.dot(ctx_ref[...], wo_ref[:, at], preferred_element_type=F32) + jnp.dot(act_ref[...], wd_ref[:, at], preferred_element_type=F32)

    @pl.when(p == 0)
    def _():
        @pl.when(t >= 3)
        def _():
            near(0, t - 3).wait_send()

        near_s[lax.rem(t, 3)] = acc_s[...].astype(BF16)
        near(0, t).start()

    @pl.when(p == 1)
    def _():
        near(0, tile).wait_recv()

        def add(at):
            recv_s[0, tile, at, :] = (acc_s[at, :] + recv_s[0, tile, at, :].astype(F32)).astype(BF16)

        by_rows(add)
        far(tile).start()

    @pl.when(p == 2)
    def _():
        @pl.when(t >= 3)
        def _():
            near(2, t - 3).wait_send()

        @pl.when(t == 0)
        def _():
            for k in range(nt - 3, nt):
                near(0, k).wait_send()

        near_s[lax.rem(t, 3)] = acc_s[...].astype(BF16)
        near(2, t).start()

    @pl.when(p == 3)
    def _():
        near(2, tile).wait_recv()
        far(tile).wait_recv()

        def add(at):
            out_ref[at, :] = (x_ref[at, :].astype(F32) + acc_s[at, :] + recv_s[2, tile, at, :].astype(F32) + recv_s[1, tile, at, :].astype(F32)).astype(BF16)

        by_rows(add)

    @pl.when(jnp.logical_and(p == 3, t == nt - 1))
    def _():
        def drain(k, carry):
            far(k).wait_send()
            return carry

        lax.fori_loop(0, nt, drain, 0)
        for k in range(nt - 3, nt):
            near(2, k).wait_send()


def back(ctx, act, wo, wd, x):
    rows, width = x.shape
    kc, kf = ctx.shape[1], act.shape[1]
    tn = 768
    nt = width // tn

    def tile_at(p, t):
        return 0, jnp.where(lax.rem(p, 2) == 0, t, nt - 1 - t)

    def last_at(p, t):
        return 0, jnp.where(p == 3, nt - 1 - t, nt - 1)

    return pl.pallas_call(
        functools.partial(back_kernel, nt),
        grid=(4, nt),
        out_shape=jax.ShapeDtypeStruct((rows, width), BF16),
        in_specs=[
            pl.BlockSpec((rows, kc), lambda p, t: (3 - p, 0)),
            pl.BlockSpec((rows, kf), lambda p, t: (3 - p, 0)),
            pl.BlockSpec((kc, tn), tile_at),
            pl.BlockSpec((kf, tn), tile_at),
            pl.BlockSpec((rows, tn), last_at),
        ],
        out_specs=pl.BlockSpec((rows, tn), last_at),
        scratch_shapes=[
            pltpu.VMEM((rows, tn), F32),
            pltpu.VMEM((3, rows, tn), BF16),
            pltpu.VMEM((3, nt, rows, tn), BF16),
            pltpu.SemaphoreType.DMA((3, nt)),
            pltpu.SemaphoreType.DMA((3, nt)),
        ],
        compiler_params=pltpu.CompilerParams(collective_id=1, has_side_effects=True, vmem_limit_bytes=VMEM_LIMIT, dimension_semantics=('arbitrary', 'arbitrary')),
        cost_estimate=pl.CostEstimate(flops=2 * 4 * rows * width * (kc + kf), bytes_accessed=4 * 2 * width * (kc + kf), transcendentals=0),
        name='back',
    )(ctx, act, wo, wd, x)


def copy_kernel(src_ref, dst_ref):
    dst_ref[...] = src_ref[...]


def hand_over(y):
    rows, width = y.shape
    tall = rows // 8
    spec = pl.BlockSpec((tall, width), lambda i: (i, 0))
    return pl.pallas_call(
        copy_kernel,
        grid=(8,),
        out_shape=jax.ShapeDtypeStruct(y.shape, y.dtype),
        in_specs=[spec],
        out_specs=spec,
        compiler_params=pltpu.CompilerParams(dimension_semantics=('arbitrary',)),
        cost_estimate=pl.CostEstimate(flops=0, bytes_accessed=4 * rows * width, transcendentals=0),
        name='hand_over',
    )(y)


def solution(mesh):
    def local_layer(hidden_blk, attn_gain, attn_bias, mlp_gain, mlp_bias, w_qkv_part, w_out_part, w_up_part, w_down_part, positions):
        width = hidden_blk.shape[-1]
        x = hidden_blk.reshape(-1, width)
        wq = jnp.transpose(w_qkv_part, (1, 2, 0)).reshape(-1, width)
        half_dim = w_qkv_part.shape[2] // 6
        cos_tab, sin_tab = rotary_tables(positions, half_dim)
        vecs = [v.reshape(1, width) for v in (attn_gain, attn_bias, mlp_gain, mlp_bias)]
        qkv, act = front(x, wq, w_up_part, *vecs)
        tp = lax.axis_index('tp').astype(jnp.int32).reshape(1)
        ctx = attention(qkv, cos_tab, sin_tab, tp)
        out = back(ctx, act, w_out_part, w_down_part, x)
        return hand_over(out).reshape(hidden_blk.shape)

    return jax.shard_map(local_layer, mesh=mesh, in_specs=(P('dp', 'tp', None), P(), P(), P(), P(), P(None, 'tp', None), P('tp', None), P(None, 'tp'), P('tp', None), P()), out_specs=P('dp', 'tp', None), check_vma=False)
```
